32 devices in a mesh: section: 2 (over x), shard: 4 (over z), replica: 4 (over y, core).
Axes of the slice: x: 2, y: 2, z: 4, core: 2. Of those that a mesh axis runs over, the one named last changes fastest.
Arguments:
- tokens: bfloat16 [3072, 2048], P(('shard', 'replica')), may hold values from -6 to 6
- targets: bfloat16 [3072, 2048], P(('shard', 'replica')), may hold values from -6 to 6
- deal: int32 [16, 192], P(('shard', 'replica')), may hold values from 0 to 191, each once within a row
- lengths: int32 [32, 2], P(('shard', 'replica')), may hold values from 24 to 48, as said below
- attn_gain: bfloat16 [2, 2048], P('section'), may hold values from 0.5 to 1.5
- w_query: bfloat16 [2, 2048, 2048], P('section', None, 'shard'), may hold values from -0.125 to 0.125
- w_key: bfloat16 [2, 2048, 512], P('section', None, 'shard'), may hold values from -0.125 to 0.125
- w_value: bfloat16 [2, 2048, 512], P('section', None, 'shard'), may hold values from -0.125 to 0.125
- w_out: bfloat16 [2, 2048, 2048], P('section', None, 'shard'), may hold values from -0.5 to 0.5
- ffn_gain: bfloat16 [2, 2048], P('section'), may hold values from 0.5 to 1.5
- w_gate: bfloat16 [2, 2048, 8192], P('section', None, 'shard'), may hold values from -0.125 to 0.125
- w_up: bfloat16 [2, 2048, 8192], P('section', None, 'shard'), may hold values from -0.125 to 0.125
- w_down: bfloat16 [2, 8192, 2048], P('section', 'shard'), may hold values from -0.09375 to 0.09375
Outputs:
- loss: float32 [], replicated
- outputs: bfloat16 [2, 3072, 2048], P('section', ('shard', 'replica'))
- input_grad: bfloat16 [2, 3072, 2048], P('section', ('shard', 'replica'))
- attn_gain_grad: float32 [2, 2048], P('section', ('shard', 'replica'))
- w_query_grad: float32 [2, 2048, 2048], P('section', 'replica', 'shard')
- w_key_grad: float32 [2, 2048, 512], P('section', 'replica', 'shard')
- w_value_grad: float32 [2, 2048, 512], P('section', 'replica', 'shard')
- w_out_grad: float32 [2, 2048, 2048], P('section', 'replica', 'shard')
- ffn_gain_grad: float32 [2, 2048], P('section', ('shard', 'replica'))
- w_gate_grad: float32 [2, 2048, 8192], P('section', 'replica', 'shard')
- w_up_grad: float32 [2, 2048, 8192], P('section', 'replica', 'shard')
- w_down_grad: float32 [2, 8192, 2048], P('section', 'shard', 'replica')
The draws below stay inside these ranges and needn't reach their ends.
Inputs may be any that keep to these rules, and one draw needn't show every extreme that they name: Each row of deal is a permutation of 0 to 191. Row b * 2 + m holds the lengths of the sequences packed, in order from row 0, into micro-batch m of token block b; the rest of the slot is padding.
All inputs are finite; a program needn't handle non-finite values.
Results may differ from the reference program's by a relative error of at most 0.028.
Values may be sent and summed in bfloat16 or wider, within the bound.
A program may use at most 256 MiB of HBM per device.

```python
import jax
import jax.numpy as jnp
from jax import lax

D = 2048
H = 32
KV = 8
HD = 64
FF = 8192
ROWS = 96
NSEQ = 2
HQ = 2048
KVD = 512
BLOCKS = 16
TOK_DEV = 192
TOKENS = 3072
SLOTS = 32


def draw_lengths(key, part):
    drawn = jax.random.randint(key, (SLOTS, NSEQ), ROWS // 4, ROWS // 2 + 1, dtype=jnp.int32)
    drawn = drawn.at[0, 0].set(ROWS // 2)
    return drawn.at[0, 1].set(ROWS // 4)


def with_spikes(values, own_key, source, target, shards_of, factor):
    owner, partner = [(jnp.arange(values.shape[axis_at]) // (values.shape[axis_at] // shards_of)).reshape([-1 if axis == axis_at else 1 for axis in range(values.ndim)]) for axis_at in (source, target)]
    chosen = jax.random.permutation(own_key, shards_of)[partner]
    strong = (owner == chosen) | (owner == (partner + shards_of // 2) % shards_of)
    return jnp.where(strong, factor * values, values)


def shard_levels(stream_key, shape, cuts, low, largest):
    loudness, own = 1.0, jax.random.fold_in(stream_key, 6)
    for dim, blocks in cuts:
        steps = jnp.exp(jax.random.uniform(jax.random.fold_in(own, dim), (blocks,), jnp.float32, low / len(cuts), largest / len(cuts)))
        loudness = loudness * jnp.repeat(steps, shape[dim] // blocks).reshape([-1 if axis == dim else 1 for axis in range(len(shape))])
    return loudness


def bell_draw(rng, shape, scale, most, pieces=(), kind=jnp.bfloat16):
    loudness = shard_levels(rng, shape, pieces, -0.22, 0.18) if pieces else 1.0
    values = jax.random.normal(rng, shape, jnp.float32) * scale * loudness
    return jnp.minimum(jnp.maximum(values, -most), most).astype(kind)


def heavy_noise(key, extent, scale, limit, split, heavy, held_as=jnp.bfloat16):
    values = scale * jax.random.normal(key, extent, jnp.float32)
    if split:
        values = values * shard_levels(key, extent, split, -0.22, 0.18)
    return jnp.clip(with_spikes(values, jax.random.fold_in(key, 3), *heavy), -limit, limit).astype(held_as)


def setup_inputs(seed: int = 0) -> dict:
    arg_keys = jax.random.split(jax.random.key(seed), 14)
    return {
        "tokens": heavy_noise(arg_keys[0], (TOKENS, D), 1.0, 6.0, ((0, 16),), (0, 1, 16, 2.0)),
        "targets": bell_draw(arg_keys[1], (TOKENS, D), 1.0, 6.0, ((0, 16),)),
        "deal": jax.vmap(lambda own: jax.random.permutation(own, TOK_DEV))(jax.random.split(arg_keys[2], BLOCKS)).reshape((BLOCKS, TOK_DEV)).astype(jnp.int32),
        "lengths": draw_lengths(jax.random.fold_in(arg_keys[13], 71), 0),
        "attn_gain": jnp.clip(1.0 + 0.1 * jax.random.normal(arg_keys[4], (2, D), jnp.float32), 0.5, 1.5).astype(jnp.bfloat16),
        "w_query": bell_draw(arg_keys[5], (2, D, HQ), D ** -0.5, 0.125, ((0, 2), (2, 4))),
        "w_key": bell_draw(arg_keys[6], (2, D, KVD), D ** -0.5, 0.125, ((0, 2), (2, 4))),
        "w_value": bell_draw(arg_keys[7], (2, D, KVD), D ** -0.5, 0.125, ((0, 2), (2, 4))),
        "w_out": bell_draw(arg_keys[8], (2, HQ, D), (HQ // 16) ** -0.5, 0.5, ((0, 2), (2, 4))),
        "ffn_gain": jnp.clip(1.0 + 0.1 * jax.random.normal(arg_keys[9], (2, D), jnp.float32), 0.5, 1.5).astype(jnp.bfloat16),
        "w_gate": bell_draw(arg_keys[10], (2, D, FF), D ** -0.5, 0.125, ((0, 2), (2, 4))),
        "w_up": bell_draw(arg_keys[11], (2, D, FF), D ** -0.5, 0.125, ((0, 2), (2, 4))),
        "w_down": bell_draw(arg_keys[12], (2, FF, D), (FF // 2) ** -0.5, 0.09375, ((0, 2), (1, 4))),
    }


EPS = 1e-05
NEG = -1e+30
ROPE_BASE = 500000.0
HIGHEST = lax.Precision.HIGHEST

@jax.custom_vjp
def low(v):
    return lax.optimization_barrier(v.astype(jnp.bfloat16)).astype(jnp.float32)

@jax.custom_vjp
def low_back(v):
    return v

def low_keep(v):
    return (low(v), None)

def low_pass(kept, grad):
    return (grad,)

def back_keep(v):
    return (v, None)

def back_low(kept, grad):
    return (low(grad),)
low.defvjp(low_keep, low_pass)
low_back.defvjp(back_keep, back_low)

def layout(seq_lengths, row_count):
    row_index = jnp.arange(row_count, dtype=jnp.int32)
    ends = jnp.cumsum(seq_lengths).astype(jnp.int32)
    segment = lax.optimization_barrier(jnp.sum((row_index[:, None] >= ends[None, :]).astype(jnp.int32), axis=1))
    begins = jnp.concatenate([jnp.zeros((1,), jnp.int32), ends])
    pick = (segment[:, None] == jnp.arange(begins.shape[0], dtype=jnp.int32)[None, :]).astype(jnp.int32)
    position = row_index - lax.optimization_barrier(jnp.sum(pick * begins[None, :], axis=1))
    return (segment, position)

def rope_tables(position, width):
    half = width // 2
    freq = ROPE_BASE ** (-2.0 * jnp.arange(half, dtype=jnp.float32) / width)
    angle = position.astype(jnp.float32)[..., None] * freq
    return (jnp.cos(angle), jnp.sin(angle))

def rotate(vector, cosine, sine):
    half = vector.shape[-1] // 2
    first_half, second_half = (vector[..., :half], vector[..., half:])
    return jnp.concatenate([first_half * cosine - second_half * sine, second_half * cosine + first_half * sine], axis=-1)

def matmul(left, right):
    return jnp.dot(left, right, precision=HIGHEST, preferred_element_type=jnp.float32)

def rms_scale(rows_in, gain):
    return rows_in * lax.rsqrt(lax.optimization_barrier(jnp.mean(rows_in * rows_in, axis=1, keepdims=True)) + EPS) * gain

def layer(rows_in, params, allowed, cosine, sine):
    attn_gain, w_query, w_key, w_value, w_out, ffn_gain, w_gate, w_up, w_down = params
    slot_count, row_count = (allowed.shape[0], allowed.shape[1])
    normed_one = low(rms_scale(rows_in, attn_gain))
    query = low_back(matmul(normed_one, w_query)).reshape(slot_count, row_count, H, HD)
    keys = low_back(matmul(normed_one, w_key)).reshape(slot_count, row_count, KV, HD)
    values = low(low_back(matmul(normed_one, w_value))).reshape(slot_count, row_count, KV, HD)
    q_rot = low(rotate(query, cosine, sine)).reshape(slot_count, row_count, KV, H // KV, HD)
    k_rot = low(rotate(keys, cosine, sine))
    scores = low_back(jnp.einsum('arkgd,askd->akgrs', q_rot, k_rot, precision=HIGHEST) * HD ** (-0.5))
    scores = jnp.where(allowed[:, None, None], scores, NEG)
    probs = low(jax.nn.softmax(scores, axis=-1))
    mixed = jnp.einsum('akgrs,askd->arkgd', probs, values, precision=HIGHEST)
    mixed = low(low_back(mixed.reshape(slot_count * row_count, H * HD)))
    hidden = rows_in + low_back(matmul(mixed, w_out))
    normed_two = low(rms_scale(hidden, ffn_gain))
    gate_pre = low_back(matmul(normed_two, w_gate))
    up_pre = low_back(matmul(normed_two, w_up))
    active = low(jax.nn.silu(gate_pre) * up_pre)
    return hidden + low_back(matmul(active, w_down))

def reference(tokens, targets, deal, lengths, attn_gain, w_query, w_key, w_value, w_out, ffn_gain, w_gate, w_up, w_down):
    block_count = deal.shape[0]
    arrival = (deal + jnp.arange(block_count, dtype=jnp.int32)[:, None] * TOK_DEV).reshape(-1).astype(jnp.int32)
    segment, position = jax.vmap(lambda seq_lengths: layout(seq_lengths, ROWS))(lengths)
    cosine, sine = rope_tables(position, HD)
    cosine, sine = (cosine[:, :, None, :], sine[:, :, None, :])
    row_index = jnp.arange(ROWS, dtype=jnp.int32)
    causal = row_index[:, None] >= row_index[None, :]
    allowed = (segment[:, :, None] == segment[:, None, :]) & causal[None]
    valid = (segment < NSEQ).reshape(-1).astype(jnp.float32)
    count = jnp.sum(lengths).astype(jnp.float32)
    teacher = targets.astype(jnp.float32)[arrival]
    inputs32 = tokens.astype(jnp.float32)
    params = tuple((w.astype(jnp.float32) for w in (attn_gain, w_query, w_key, w_value, w_out, ffn_gain, w_gate, w_up, w_down)))
    nudge = jnp.zeros((TOKENS, D), jnp.float32)

    def objective(inputs_all, weights_all, nudge_rows):
        first_out = layer(inputs_all[arrival], [w[0] for w in weights_all], allowed, cosine, sine)
        second_in = low(low_back(first_out + nudge_rows))
        second_out = layer(second_in, [w[1] for w in weights_all], allowed, cosine, sine)
        errors = second_out - teacher
        loss_value = jnp.sum(valid[:, None] * errors * errors) / (count * D)
        return (loss_value * (D * TOKENS / 2.0), (first_out, second_out, loss_value))
    scaled, backward, aux = jax.vjp(objective, inputs32, params, nudge, has_aux=True)
    first_out, second_out, loss_value = aux
    grad_inputs, grad_params, grad_nudge = backward(jnp.ones_like(scaled))

    def to_arrival(slot_rows):
        return jnp.zeros((TOKENS, D), jnp.float32).at[arrival].set(slot_rows).astype(jnp.bfloat16)
    outputs = jnp.stack([to_arrival(first_out), to_arrival(second_out)])
    input_grad = jnp.stack([grad_inputs.astype(jnp.bfloat16), to_arrival(grad_nudge)])
    return (loss_value, outputs, input_grad, grad_params[0], grad_params[1], grad_params[2], grad_params[3], grad_params[4], grad_params[5], grad_params[6], grad_params[7], grad_params[8])
```

```python
import functools

import jax
import jax.numpy as jnp
from jax import lax
from jax.experimental import pallas as pl
from jax.experimental.pallas import tpu as pltpu
from jax.sharding import PartitionSpec as P

H = 32
KV = 8
HD = 64


EPS = 1e-05
NEG = -1e30
ROPE_BASE = 500000.0
MESH = pl.DeviceIdType.MESH
ANY = pl.BlockSpec(memory_space=pl.ANY)
VM = pl.BlockSpec(memory_space=pltpu.VMEM)


def from_behind(block, axis, distance):
    devices = range(lax.axis_size(axis))
    route = [(i - distance, i) for i in devices if i - distance in devices]
    return lax.ppermute(block, axis, route)


def layout(seq_lengths, row_count):
    row_index = jnp.arange(row_count, dtype=jnp.int32)
    ends = jnp.cumsum(seq_lengths)
    segment = jnp.sum((row_index[:, None] >= ends[None, :]).astype(jnp.int32), axis=1)
    begins = jnp.concatenate([jnp.zeros((1,), jnp.int32), ends])
    pick = (segment[:, None] == jnp.arange(begins.shape[0], dtype=jnp.int32)[None, :]).astype(
        jnp.int32
    )
    position = row_index - jnp.sum(pick * begins[None, :], axis=1)
    return (segment, position)


def rope_tables(position, width):
    half = width // 2
    freq = ROPE_BASE ** (-2.0 * jnp.arange(half, dtype=jnp.float32) / width)
    angle = position.astype(jnp.float32)[..., None] * freq
    return (jnp.cos(angle), jnp.sin(angle))


def rotate(vector, cosine, sine):
    half = vector.shape[-1] // 2
    first_half, second_half = (vector[..., :half], vector[..., half:])
    return jnp.concatenate(
        [first_half * cosine - second_half * sine, second_half * cosine + first_half * sine],
        axis=-1,
    )


def rotate_back(grad, cosine, sine):
    half = grad.shape[-1] // 2
    first_half, second_half = (grad[..., :half], grad[..., half:])
    return jnp.concatenate(
        [first_half * cosine + second_half * sine, second_half * cosine - first_half * sine],
        axis=-1,
    )


def across(left, right):
    return lax.dot_general(
        left, right, (((1,), (1,)), ((), ())), preferred_element_type=jnp.float32
    )


def down_rows(left, right):
    return lax.dot_general(
        left, right, (((0,), (0,)), ((), ())), preferred_element_type=jnp.float32
    )


def attend_mask(seq_lengths, row_count):
    segment, position = layout(seq_lengths, row_count)
    row_index = jnp.arange(row_count, dtype=jnp.int32)
    allowed = (segment[:, None] == segment[None, :]) & (row_index[:, None] >= row_index[None, :])
    cosine, sine = rope_tables(position, HD)
    return (allowed, cosine[:, None, :], sine[:, None, :])


def place():
    return (lax.axis_index("section"), lax.axis_index("shard"), lax.axis_index("replica"))


def reduce_peers(n_rep):
    section, shard, replica = place()
    peers = []
    bit = 1
    while bit < n_rep:
        peers.append((section, shard, replica ^ bit))
        bit *= 2
    peers.append((section, shard ^ 1, replica))
    peers.append((section, 3 - shard, replica))
    return peers


def greet(peers):
    barrier = pltpu.get_barrier_semaphore()
    for peer in peers:
        pl.semaphore_signal(barrier, inc=1, device_id=peer, device_id_type=MESH)
    pl.semaphore_wait(barrier, len(peers))


def butterfly(peers, totals, heard, send_sem, recv_sem):
    for step, peer in enumerate(peers):
        copy = pltpu.make_async_remote_copy(
            src_ref=totals.at[step],
            dst_ref=heard.at[step],
            send_sem=send_sem.at[step],
            recv_sem=recv_sem.at[step],
            device_id=peer,
            device_id_type=MESH,
        )
        copy.start()
        copy.wait()
        totals[step + 1] = totals[step] + heard[step]


def gather_kernel(
    n_rep,
    count_ref,
    in_q,
    in_o,
    in_k,
    in_v,
    count_out,
    out_q,
    out_o,
    out_k,
    out_v,
    own_q,
    own_o,
    own_k,
    own_v,
    totals,
    heard,
    bf_send,
    bf_recv,
    load_sem,
    send_z,
    recv_z,
    send_y,
    recv_y,
    send_c,
    recv_c,
):
    section, shard, replica = place()
    ins = (in_q, in_o, in_k, in_v)
    outs = (out_q, out_o, out_k, out_v)
    owns = (own_q, own_o, own_k, own_v)
    quarter_rows = in_q.shape[0] // 4
    mine = lax.rem(replica, 4)
    peers = reduce_peers(n_rep)
    sibling = (section, shard, replica ^ 1)
    across_y = (section, shard, replica ^ 2)
    greet(peers)

    def rows(quarter):
        return pl.ds(pl.multiple_of(quarter * quarter_rows, 128), quarter_rows)

    def piece(index, source, quarter):
        width = ins[index].shape[1]
        return outs[index].at[rows(quarter), pl.ds(pl.multiple_of(source * width, 128), width)]

    def along_z(index, source, step):
        side = (step + 1) // 2
        from_ref = piece(index, source, mine)
        return pltpu.make_async_remote_copy(
            src_ref=from_ref,
            dst_ref=from_ref,
            send_sem=send_z.at[side, index, source],
            recv_sem=recv_z.at[index, source],
            device_id=(section, shard + step, replica),
            device_id_type=MESH,
        )

    def first_z(index, step):
        side = (step + 1) // 2
        return pltpu.make_async_remote_copy(
            src_ref=ins[index].at[rows(mine), :],
            dst_ref=piece(index, shard, mine),
            send_sem=send_z.at[side, index, shard],
            recv_sem=recv_z.at[index, shard],
            device_id=(section, shard + step, replica),
            device_id_type=MESH,
        )

    def to_y(index, source, quarter):
        ref = piece(index, source, quarter)
        return pltpu.make_async_remote_copy(
            src_ref=ref,
            dst_ref=ref,
            send_sem=send_y.at[index, source],
            recv_sem=recv_y.at[index, source],
            device_id=across_y,
            device_id_type=MESH,
        )

    def to_core(index, source, quarter, which):
        ref = piece(index, source, quarter)
        return pltpu.make_async_remote_copy(
            src_ref=ref,
            dst_ref=ref,
            send_sem=send_c.at[which, index, source],
            recv_sem=recv_c.at[which, index, source],
            device_id=sibling,
            device_id_type=MESH,
        )

    for index in range(4):
        for step in (-1, 1):

            @pl.when((shard + step >= 0) & (shard + step < 4))
            def _():
                first_z(index, step).start()

    loads = [
        pltpu.make_async_copy(ins[index], owns[index], load_sem.at[index]) for index in range(4)
    ]
    for load in loads:
        load.start()
    totals[0] = count_ref[...]
    butterfly(peers, totals, heard, bf_send, bf_recv)
    count_out[...] = totals[len(peers)]
    stores = []
    for index in range(4):
        loads[index].wait()
        width = ins[index].shape[1]
        store = pltpu.make_async_copy(
            owns[index],
            outs[index].at[:, pl.ds(pl.multiple_of(shard * width, 128), width)],
            load_sem.at[index],
        )
        store.start()
        stores.append(store)

    items = [(d, index, side) for d in (1, 2, 3) for index in range(4) for side in (-1, 1)]
    for place_in_line in range(len(items) + 1):
        if place_in_line < len(items):
            d, index, side = items[place_in_line]
            source = shard + side * d

            @pl.when((source >= 0) & (source < 4))
            def _():
                along_z(index, source, -side).wait_recv()

                @pl.when((shard - side >= 0) & (shard - side < 4))
                def _():
                    along_z(index, source, -side).start()

                to_y(index, source, mine).start()
                to_core(index, source, mine, 0).start()

        if place_in_line > 0:
            d, index, side = items[place_in_line - 1]
            source = shard + side * d

            @pl.when((source >= 0) & (source < 4))
            def _():
                to_y(index, source, mine ^ 2).wait_recv()
                to_core(index, source, mine ^ 2, 1).start()

    for d, index, side in items:
        source = shard + side * d

        @pl.when((source >= 0) & (source < 4))
        def _():
            to_core(index, source, mine ^ 1, 0).wait_recv()
            to_core(index, source, mine ^ 3, 1).wait_recv()
            to_y(index, source, mine).wait_send()
            to_core(index, source, mine, 0).wait_send()
            to_core(index, source, mine ^ 2, 1).wait_send()

            @pl.when((shard - side >= 0) & (shard - side < 4))
            def _():
                along_z(index, source, -side).wait_send()

    for index in range(4):
        for step in (-1, 1):

            @pl.when((shard + step >= 0) & (shard + step < 4))
            def _():
                first_z(index, step).wait_send()

        stores[index].wait()


def gather_weights(n_rep, count, w_q, w_o, w_k, w_v):
    weights = (w_q, w_o, w_k, w_v)
    steps = n_rep.bit_length() - 1 + 2
    bf16, f32 = jnp.bfloat16, jnp.float32
    dma = pltpu.SemaphoreType.DMA
    return pl.pallas_call(
        functools.partial(gather_kernel, n_rep),
        out_shape=(jax.ShapeDtypeStruct(count.shape, f32),)
        + tuple(jax.ShapeDtypeStruct((w.shape[0], w.shape[1] * 4), bf16) for w in weights),
        in_specs=[VM] + [ANY] * 4,
        out_specs=(VM,) + (ANY,) * 4,
        scratch_shapes=[pltpu.VMEM(w.shape, bf16) for w in weights]
        + [
            pltpu.VMEM((steps + 1,) + count.shape, f32),
            pltpu.VMEM((steps,) + count.shape, f32),
            dma((steps,)),
            dma((steps,)),
            dma((4,)),
            dma((2, 4, 4)),
            dma((4, 4)),
            dma((4, 4)),
            dma((4, 4)),
            dma((2, 4, 4)),
            dma((2, 4, 4)),
        ],
        compiler_params=pltpu.CompilerParams(
            collective_id=0, has_side_effects=True, vmem_limit_bytes=16 << 20
        ),
        name="gather_weights",
    )(count, *weights)


def sum_kernel(n_rep, part_ref, group_out, whole_out, totals, heard, send_sem, recv_sem):
    section, shard, replica = place()
    peers = reduce_peers(n_rep) + [(1 - section, shard, replica)]
    greet(peers)
    totals[0] = part_ref[...]
    butterfly(peers, totals, heard, send_sem, recv_sem)
    group_out[...] = totals[len(peers) - 1]
    whole_out[...] = totals[len(peers)]


def small_sums(n_rep, part):
    steps = n_rep.bit_length() - 1 + 3
    shape = jax.ShapeDtypeStruct(part.shape, jnp.float32)
    return pl.pallas_call(
        functools.partial(sum_kernel, n_rep),
        out_shape=(shape, shape),
        in_specs=[VM],
        out_specs=(VM, VM),
        scratch_shapes=[
            pltpu.VMEM((steps + 1,) + part.shape, jnp.float32),
            pltpu.VMEM((steps,) + part.shape, jnp.float32),
            pltpu.SemaphoreType.DMA((steps,)),
            pltpu.SemaphoreType.DMA((steps,)),
        ],
        compiler_params=pltpu.CompilerParams(
            collective_id=1, has_side_effects=True, vmem_limit_bytes=8 << 20
        ),
        name="small_sums",
    )(part)


def flip(block, bit):
    size = lax.axis_size("replica")
    return lax.ppermute(block, "replica", [(i, i ^ bit) for i in range(size)])


def owned(left, right, split):
    size = lax.axis_size("replica")
    me = lax.axis_index("replica")
    divided = right if split else left
    length = divided.shape[1] // size
    blocks = divided.reshape(divided.shape[0], size // 2, 2, length)

    def product(which):
        chosen = lax.dynamic_index_in_dim(blocks, which, 2, keepdims=False)
        chosen = chosen.reshape(divided.shape[0], -1)
        if split:
            total = down_rows(left, chosen)
            return total
        return down_rows(chosen, right)

    sent = product(1 - (me & 1)).astype(jnp.bfloat16)
    arrived = flip(sent, 1)
    total = product(me & 1) + arrived.astype(jnp.float32)
    bit = 2
    while bit < size:
        here = (me // bit) & 1
        if split:
            halves = total.reshape(total.shape[0], -1, 2, length)
        else:
            halves = total.reshape(-1, 2, length, total.shape[1])
        axis = 2 if split else 1
        away = lax.dynamic_index_in_dim(halves, 1 - here, axis, keepdims=False)
        keep = lax.dynamic_index_in_dim(halves, here, axis, keepdims=False)
        arrived = flip(away.astype(jnp.bfloat16), bit)
        total = keep + arrived.astype(jnp.float32)
        total = total.reshape((total.shape[0], -1) if split else (-1, total.shape[-1]))
        bit *= 2
    return total


def over_shard(grad):
    return lax.psum_scatter(
        grad.astype(jnp.bfloat16), "shard", scatter_dimension=1, tiled=True
    ).astype(jnp.float32)


def per_device(
    tokens,
    targets,
    deal,
    lengths,
    attn_gain,
    w_query,
    w_key,
    w_value,
    w_out,
    ffn_gain,
    w_gate,
    w_up,
    w_down,
):
    f32 = jnp.float32
    bf16 = jnp.bfloat16
    n_rep = lax.axis_size("replica")
    section_id = lax.axis_index("section")
    later = section_id == 1
    micro_count = lengths.shape[0]
    row_count = tokens.shape[0] // micro_count
    model_width = tokens.shape[1]
    group_size = H // KV
    score_scale = HD ** (-0.5)
    arrival = deal[0]
    slot_inputs = tokens[arrival].reshape(micro_count, row_count, model_width)
    teacher = targets[arrival].astype(f32)
    gain_attn = attn_gain[0].astype(f32)
    gain_ffn = ffn_gain[0].astype(f32)
    local_count = jnp.broadcast_to(jnp.sum(lengths).astype(f32), (8, 128))
    counted, w_q, w_o, w_k, w_v = gather_weights(
        n_rep, local_count, w_query[0], w_out[0], w_key[0], w_value[0]
    )
    total_count = counted[0, 0]
    w_g, w_u, w_d = (w_gate[0], w_up[0], w_down[0])
    received = jnp.zeros((row_count, model_width), bf16)
    outputs_seen = []
    kept_seen = []

    def pick(one, zero):
        return jax.tree.map(lambda a, b: jnp.where(later, a, b), one, zero)

    for moment in range(micro_count + 1):
        own_batch = jnp.clip(moment - section_id, 0, micro_count - 1)
        fresh = lax.dynamic_index_in_dim(slot_inputs, own_batch, 0, keepdims=False)
        seq_lengths = lax.dynamic_index_in_dim(lengths, own_batch, 0, keepdims=False)
        rows_in = jnp.where(later, received, fresh).astype(f32)
        forward_allowed, forward_cosine, forward_sine = attend_mask(seq_lengths, row_count)
        forward_inverse_one = lax.rsqrt(jnp.mean(rows_in * rows_in, axis=1, keepdims=True) + EPS)
        forward_normed_one = (rows_in * forward_inverse_one * gain_attn).astype(bf16)
        query = jnp.dot(forward_normed_one, w_q, preferred_element_type=f32).reshape(
            row_count, H, HD
        )
        keys = jnp.dot(forward_normed_one, w_k, preferred_element_type=f32).reshape(
            row_count, KV, HD
        )
        forward_values = (
            jnp.dot(forward_normed_one, w_v, preferred_element_type=f32)
            .astype(bf16)
            .reshape(row_count, KV, HD)
        )
        forward_q_rot = (
            rotate(query, forward_cosine, forward_sine)
            .astype(bf16)
            .reshape(row_count, KV, group_size, HD)
        )
        forward_k_rot = rotate(keys, forward_cosine, forward_sine).astype(bf16)
        forward_scores = (
            jnp.einsum("rkgd,skd->kgrs", forward_q_rot, forward_k_rot, preferred_element_type=f32)
            * score_scale
        )
        forward_scores = jnp.where(forward_allowed, forward_scores, NEG)
        highest = jnp.max(forward_scores, axis=-1, keepdims=True)
        raised = jnp.exp(forward_scores - highest)
        totals = jnp.sum(raised, axis=-1, keepdims=True)
        forward_probs = (raised / totals).astype(bf16)
        forward_log_total = highest + jnp.log(totals)
        forward_mixed = jnp.einsum(
            "kgrs,skd->rkgd", forward_probs, forward_values, preferred_element_type=f32
        )
        forward_mixed = forward_mixed.reshape(row_count, H * HD).astype(bf16)
        forward_hidden = rows_in + jnp.dot(forward_mixed, w_o, preferred_element_type=f32)
        forward_inverse_two = lax.rsqrt(
            jnp.mean(forward_hidden * forward_hidden, axis=1, keepdims=True) + EPS
        )
        forward_normed_two = (forward_hidden * forward_inverse_two * gain_ffn).astype(bf16)
        ffn_spread = lax.all_gather(forward_normed_two, "shard", axis=0, tiled=True)
        ffn_gate_pre = jnp.dot(ffn_spread, w_g, preferred_element_type=f32)
        ffn_up_pre = jnp.dot(ffn_spread, w_u, preferred_element_type=f32)
        ffn_active = (jax.nn.silu(ffn_gate_pre) * ffn_up_pre).astype(bf16)
        branch = lax.psum_scatter(
            jnp.dot(ffn_active, w_d, preferred_element_type=f32).astype(jnp.bfloat16),
            "shard",
            scatter_dimension=0,
            tiled=True,
        ).astype(jnp.float32)
        forward_kept = (
            rows_in.astype(bf16),
            forward_inverse_one,
            forward_normed_one,
            forward_q_rot,
            forward_k_rot,
            forward_values,
            forward_log_total,
            forward_mixed,
            forward_hidden,
            forward_inverse_two,
            ffn_spread,
            ffn_gate_pre.astype(bf16),
            ffn_up_pre.astype(bf16),
            ffn_active,
        )
        result = forward_hidden + branch
        kept = forward_kept
        if moment < micro_count:
            received = from_behind(result.astype(bf16), "section", 1)
        outputs_seen.append(result)
        kept_seen.append(kept)
    mine = jnp.concatenate(
        [pick(outputs_seen[batch + 1], outputs_seen[batch]) for batch in range(micro_count)]
    )
    segments_all = jax.vmap(lambda seq_lengths: layout(seq_lengths, row_count)[0])(lengths)
    valid_rows = (segments_all < lengths.shape[1]).reshape(-1).astype(f32)[:, None]
    errors = mine - teacher
    switch = later.astype(f32)
    local_square = jnp.sum(valid_rows * errors * errors) * switch
    all_tokens = tokens.shape[0] * lax.axis_size("shard") * lax.axis_size("replica")
    grad_final = (all_tokens / total_count * errors * valid_rows).reshape(
        micro_count, row_count, model_width
    )
    coming = jnp.zeros((row_count, model_width), bf16)
    sent_seen = []
    stored_seen = []
    gain_attn_total = jnp.zeros((model_width,), f32)
    gain_ffn_total = jnp.zeros((model_width,), f32)
    for moment in range(micro_count + 1):
        raw_batch = moment - 1 + section_id
        own_batch = jnp.clip(raw_batch, 0, micro_count - 1)
        if moment == 1:
            kept = pick(kept_seen[2], kept_seen[0])
        else:
            kept = kept_seen[1]
        seq_lengths = lax.dynamic_index_in_dim(lengths, own_batch, 0, keepdims=False)
        final_rows = lax.dynamic_index_in_dim(grad_final, own_batch, 0, keepdims=False)
        incoming = jnp.where(later, final_rows, coming.astype(f32))
        (
            input_rows,
            inverse_one,
            normed_one,
            q_rot,
            k_rot,
            values,
            log_total,
            mixed,
            hidden,
            inverse_two,
            spread,
            gate_pre,
            up_pre,
            active,
        ) = kept
        gate_pre, up_pre = gate_pre.astype(f32), up_pre.astype(f32)
        allowed, cosine, sine = attend_mask(seq_lengths, row_count)
        grad_branch = incoming.astype(bf16)
        backward_grad_rows = lax.all_gather(grad_branch, "shard", axis=0, tiled=True)
        grad_active = across(backward_grad_rows, w_d)
        sigma = jax.nn.sigmoid(gate_pre)
        backward_grad_gate = (
            grad_active * up_pre * sigma * (1.0 + gate_pre * (1.0 - sigma))
        ).astype(bf16)
        backward_grad_up = (grad_active * gate_pre * sigma).astype(bf16)
        grad_normed = lax.psum_scatter(
            (across(backward_grad_gate, w_g) + across(backward_grad_up, w_u)).astype(jnp.bfloat16),
            "shard",
            scatter_dimension=0,
            tiled=True,
        ).astype(jnp.float32)
        scaled_two = hidden * inverse_two
        gain_ffn_part = jnp.sum(grad_normed * scaled_two, axis=0)
        pushed_two = grad_normed * gain_ffn
        grad_hidden = incoming + inverse_two * (
            pushed_two - scaled_two * jnp.mean(pushed_two * scaled_two, axis=1, keepdims=True)
        )
        backward_grad_attn = grad_hidden.astype(bf16)
        grad_mixed = (
            across(backward_grad_attn, w_o).astype(bf16).reshape(row_count, KV, group_size, HD)
        )
        scores = (
            jnp.einsum("rkgd,skd->kgrs", q_rot, k_rot, preferred_element_type=f32) * score_scale
        )
        probs = jnp.where(allowed, jnp.exp(scores - log_total), 0.0)
        grad_probs = jnp.einsum("rkgd,skd->kgrs", grad_mixed, values, preferred_element_type=f32)
        grad_scores = (
            probs * (grad_probs - jnp.sum(grad_probs * probs, axis=-1, keepdims=True))
        ).astype(bf16)
        grad_qrot = (
            jnp.einsum("kgrs,skd->rkgd", grad_scores, k_rot, preferred_element_type=f32)
            * score_scale
        )
        grad_krot = (
            jnp.einsum("kgrs,rkgd->skd", grad_scores, q_rot, preferred_element_type=f32)
            * score_scale
        )
        backward_grad_values = jnp.einsum(
            "kgrs,rkgd->skd", probs.astype(bf16), grad_mixed, preferred_element_type=f32
        )
        backward_grad_values = backward_grad_values.astype(bf16).reshape(row_count, KV * HD)
        backward_grad_query = (
            rotate_back(grad_qrot.reshape(row_count, H, HD), cosine, sine)
            .astype(bf16)
            .reshape(row_count, H * HD)
        )
        backward_grad_keys = (
            rotate_back(grad_krot, cosine, sine).astype(bf16).reshape(row_count, KV * HD)
        )
        grad_normed_one = (
            across(backward_grad_query, w_q)
            + across(backward_grad_keys, w_k)
            + across(backward_grad_values, w_v)
        )
        scaled_one = input_rows.astype(f32) * inverse_one
        gain_attn_part = jnp.sum(grad_normed_one * scaled_one, axis=0)
        pushed_one = grad_normed_one * gain_attn
        grad_input = grad_hidden + inverse_one * (
            pushed_one - scaled_one * jnp.mean(pushed_one * scaled_one, axis=1, keepdims=True)
        )
        stored = (
            normed_one,
            backward_grad_query,
            backward_grad_keys,
            backward_grad_values,
            mixed,
            backward_grad_attn,
            spread,
            backward_grad_gate,
            backward_grad_up,
            backward_grad_rows,
            active,
        )
        active_moment = (raw_batch >= 0) & (raw_batch < micro_count)
        gain_attn_total = gain_attn_total + jnp.where(active_moment, gain_attn_part, 0.0)
        gain_ffn_total = gain_ffn_total + jnp.where(active_moment, gain_ffn_part, 0.0)
        sent = grad_input.astype(bf16)
        if moment < micro_count:
            coming = from_behind(sent, "section", -1)
        sent_seen.append(sent)
        stored_seen.append(stored)
    grads_in = jnp.concatenate(
        [pick(sent_seen[batch], sent_seen[batch + 1]) for batch in range(micro_count)]
    )
    stored_valid = jax.tree.map(
        lambda both, other: jnp.concatenate([both, other]),
        stored_seen[1],
        pick(stored_seen[0], stored_seen[2]),
    )
    (
        normed_rows,
        grad_query,
        grad_keys,
        grad_values,
        mixed_rows,
        grad_attn,
        spread_rows,
        grad_gate,
        grad_up,
        grad_rows,
        active_rows,
    ) = stored_valid
    down_grad = owned(active_rows, grad_rows, 1)
    gate_grad = owned(spread_rows, grad_gate, 0)
    up_grad = owned(spread_rows, grad_up, 0)
    out_grad = over_shard(owned(mixed_rows, grad_attn, 0))
    query_grad = over_shard(owned(normed_rows, grad_query, 0))
    key_grad = over_shard(owned(normed_rows, grad_keys, 0))
    value_grad = over_shard(owned(normed_rows, grad_values, 0))
    small = jnp.stack([gain_attn_total, gain_ffn_total])
    small = jnp.concatenate([small, jnp.broadcast_to(local_square, (6, model_width))])
    group_sums, whole_sums = small_sums(n_rep, small)
    loss_value = whole_sums[2, 0] / (total_count * model_width)
    share = model_width // (lax.axis_size("shard") * n_rep)
    start = (lax.axis_index("shard") * n_rep + lax.axis_index("replica")) * share
    attn_gain_part = lax.dynamic_slice_in_dim(group_sums[0], start, share, 0)
    ffn_gain_part = lax.dynamic_slice_in_dim(group_sums[1], start, share, 0)
    outputs_local = (
        jnp.zeros((tokens.shape[0], model_width), bf16).at[arrival].set(mine.astype(bf16))[None]
    )
    input_local = jnp.zeros((tokens.shape[0], model_width), bf16).at[arrival].set(grads_in)[None]
    return (
        loss_value,
        outputs_local,
        input_local,
        attn_gain_part[None],
        query_grad[None],
        key_grad[None],
        value_grad[None],
        out_grad[None],
        ffn_gain_part[None],
        gate_grad[None],
        up_grad[None],
        down_grad[None],
    )


def solution(mesh):
    in_specs = (
        P(("shard", "replica"), None),
        P(("shard", "replica"), None),
        P(("shard", "replica"), None),
        P(("shard", "replica"), None),
        P("section", None),
        P("section", None, "shard"),
        P("section", None, "shard"),
        P("section", None, "shard"),
        P("section", None, "shard"),
        P("section", None),
        P("section", None, "shard"),
        P("section", None, "shard"),
        P("section", "shard", None),
    )
    out_specs = (
        P(),
        P("section", ("shard", "replica"), None),
        P("section", ("shard", "replica"), None),
        P("section", ("shard", "replica")),
        P("section", "replica", "shard"),
        P("section", "replica", "shard"),
        P("section", "replica", "shard"),
        P("section", "replica", "shard"),
        P("section", ("shard", "replica")),
        P("section", "replica", "shard"),
        P("section", "replica", "shard"),
        P("section", "shard", "replica"),
    )
    return jax.shard_map(
        per_device, mesh=mesh, in_specs=in_specs, out_specs=out_specs, check_vma=False
    )
```

```python
import functools

import jax
import jax.numpy as jnp
from jax import lax
from jax.experimental import pallas as pl
from jax.experimental.pallas import tpu as pltpu
from jax.sharding import PartitionSpec as P

H = 32
KV = 8
HD = 64


EPS = 1e-05
NEG = -1e30
ROPE_BASE = 500000.0
MESH = pl.DeviceIdType.MESH
ANY = pl.BlockSpec(memory_space=pl.ANY)
VM = pl.BlockSpec(memory_space=pltpu.VMEM)


def from_behind(block, axis, distance):
    devices = range(lax.axis_size(axis))
    route = [(i - distance, i) for i in devices if i - distance in devices]
    return lax.ppermute(block, axis, route)


def layout(seq_lengths, row_count):
    row_index = jnp.arange(row_count, dtype=jnp.int32)
    ends = jnp.cumsum(seq_lengths)
    segment = jnp.sum((row_index[:, None] >= ends[None, :]).astype(jnp.int32), axis=1)
    begins = jnp.concatenate([jnp.zeros((1,), jnp.int32), ends])
    pick = (segment[:, None] == jnp.arange(begins.shape[0], dtype=jnp.int32)[None, :]).astype(
        jnp.int32
    )
    position = row_index - jnp.sum(pick * begins[None, :], axis=1)
    return (segment, position)


def rope_tables(position, width):
    half = width // 2
    freq = ROPE_BASE ** (-2.0 * jnp.arange(half, dtype=jnp.float32) / width)
    angle = position.astype(jnp.float32)[..., None] * freq
    return (jnp.cos(angle), jnp.sin(angle))


def rotate(vector, cosine, sine):
    half = vector.shape[-1] // 2
    first_half, second_half = (vector[..., :half], vector[..., half:])
    return jnp.concatenate(
        [first_half * cosine - second_half * sine, second_half * cosine + first_half * sine],
        axis=-1,
    )


def rotate_back(grad, cosine, sine):
    half = grad.shape[-1] // 2
    first_half, second_half = (grad[..., :half], grad[..., half:])
    return jnp.concatenate(
        [first_half * cosine + second_half * sine, second_half * cosine - first_half * sine],
        axis=-1,
    )


def across(left, right):
    return lax.dot_general(
        left, right, (((1,), (1,)), ((), ())), preferred_element_type=jnp.float32
    )


def down_rows(left, right):
    return lax.dot_general(
        left, right, (((0,), (0,)), ((), ())), preferred_element_type=jnp.float32
    )


def attend_mask(seq_lengths, row_count):
    segment, position = layout(seq_lengths, row_count)
    row_index = jnp.arange(row_count, dtype=jnp.int32)
    allowed = (segment[:, None] == segment[None, :]) & (row_index[:, None] >= row_index[None, :])
    cosine, sine = rope_tables(position, HD)
    return (allowed, cosine[:, None, :], sine[:, None, :])


def place():
    return (lax.axis_index("section"), lax.axis_index("shard"), lax.axis_index("replica"))


def reduce_peers(n_rep):
    section, shard, replica = place()
    peers = []
    bit = 1
    while bit < n_rep:
        peers.append((section, shard, replica ^ bit))
        bit *= 2
    peers.append((section, shard ^ 1, replica))
    peers.append((section, 3 - shard, replica))
    return peers


def greet(peers):
    barrier = pltpu.get_barrier_semaphore()
    for peer in peers:
        pl.semaphore_signal(barrier, inc=1, device_id=peer, device_id_type=MESH)
    pl.semaphore_wait(barrier, len(peers))


def butterfly(peers, totals, heard, send_sem, recv_sem):
    for step, peer in enumerate(peers):
        copy = pltpu.make_async_remote_copy(
            src_ref=totals.at[step],
            dst_ref=heard.at[step],
            send_sem=send_sem.at[step],
            recv_sem=recv_sem.at[step],
            device_id=peer,
            device_id_type=MESH,
        )
        copy.start()
        copy.wait()
        totals[step + 1] = totals[step] + heard[step]


def gather_kernel(
    n_rep,
    count_ref,
    in_q,
    in_o,
    in_k,
    in_v,
    count_out,
    out_q,
    out_o,
    out_k,
    out_v,
    own_q,
    own_o,
    own_k,
    own_v,
    totals,
    heard,
    bf_send,
    bf_recv,
    load_sem,
    send_z,
    recv_z,
    send_y,
    recv_y,
    send_c,
    recv_c,
):
    section, shard, replica = place()
    ins = (in_q, in_o, in_k, in_v)
    outs = (out_q, out_o, out_k, out_v)
    owns = (own_q, own_o, own_k, own_v)
    quarter_rows = in_q.shape[0] // 4
    mine = lax.rem(replica, 4)
    peers = reduce_peers(n_rep)
    sibling = (section, shard, replica ^ 1)
    across_y = (section, shard, replica ^ 2)
    greet(peers)

    def rows(quarter):
        return pl.ds(pl.multiple_of(quarter * quarter_rows, 128), quarter_rows)

    def piece(index, source, quarter):
        width = ins[index].shape[1]
        return outs[index].at[rows(quarter), pl.ds(pl.multiple_of(source * width, 128), width)]

    def along_z(index, source, step):
        side = (step + 1) // 2
        from_ref = piece(index, source, mine)
        return pltpu.make_async_remote_copy(
            src_ref=from_ref,
            dst_ref=from_ref,
            send_sem=send_z.at[side, index, source],
            recv_sem=recv_z.at[index, source],
            device_id=(section, shard + step, replica),
            device_id_type=MESH,
        )

    def first_z(index, step):
        side = (step + 1) // 2
        return pltpu.make_async_remote_copy(
            src_ref=ins[index].at[rows(mine), :],
            dst_ref=piece(index, shard, mine),
            send_sem=send_z.at[side, index, shard],
            recv_sem=recv_z.at[index, shard],
            device_id=(section, shard + step, replica),
            device_id_type=MESH,
        )

    def to_y(index, source, quarter):
        ref = piece(index, source, quarter)
        return pltpu.make_async_remote_copy(
            src_ref=ref,
            dst_ref=ref,
            send_sem=send_y.at[index, source],
            recv_sem=recv_y.at[index, source],
            device_id=across_y,
            device_id_type=MESH,
        )

    def to_core(index, source, quarter, which):
        ref = piece(index, source, quarter)
        return pltpu.make_async_remote_copy(
            src_ref=ref,
            dst_ref=ref,
            send_sem=send_c.at[which, index, source],
            recv_sem=recv_c.at[which, index, source],
            device_id=sibling,
            device_id_type=MESH,
        )

    for index in range(4):
        for step in (-1, 1):

            @pl.when((shard + step >= 0) & (shard + step < 4))
            def _():
                first_z(index, step).start()

    loads = [
        pltpu.make_async_copy(ins[index], owns[index], load_sem.at[index]) for index in range(4)
    ]
    for load in loads:
        load.start()
    totals[0] = count_ref[...]
    butterfly(peers, totals, heard, bf_send, bf_recv)
    count_out[...] = totals[len(peers)]
    stores = []
    for index in range(4):
        loads[index].wait()
        width = ins[index].shape[1]
        store = pltpu.make_async_copy(
            owns[index],
            outs[index].at[:, pl.ds(pl.multiple_of(shard * width, 128), width)],
            load_sem.at[index],
        )
        store.start()
        stores.append(store)

    items = [(d, index, side) for d in (1, 2, 3) for index in range(4) for side in (-1, 1)]
    lag = 8
    for place_in_line in range(len(items) + lag):
        if place_in_line < len(items):
            d, index, side = items[place_in_line]
            source = shard + side * d

            @pl.when((source >= 0) & (source < 4))
            def _():
                along_z(index, source, -side).wait_recv()

                @pl.when((shard - side >= 0) & (shard - side < 4))
                def _():
                    along_z(index, source, -side).start()

                to_y(index, source, mine).start()
                to_core(index, source, mine, 0).start()

        if place_in_line >= lag:
            d, index, side = items[place_in_line - lag]
            source = shard + side * d

            @pl.when((source >= 0) & (source < 4))
            def _():
                to_y(index, source, mine ^ 2).wait_recv()
                to_core(index, source, mine ^ 2, 1).start()

    for d, index, side in items:
        source = shard + side * d

        @pl.when((source >= 0) & (source < 4))
        def _():
            to_core(index, source, mine ^ 1, 0).wait_recv()
            to_core(index, source, mine ^ 3, 1).wait_recv()
            to_y(index, source, mine).wait_send()
            to_core(index, source, mine, 0).wait_send()
            to_core(index, source, mine ^ 2, 1).wait_send()

            @pl.when((shard - side >= 0) & (shard - side < 4))
            def _():
                along_z(index, source, -side).wait_send()

    for index in range(4):
        for step in (-1, 1):

            @pl.when((shard + step >= 0) & (shard + step < 4))
            def _():
                first_z(index, step).wait_send()

        stores[index].wait()


def gather_weights(n_rep, count, w_q, w_o, w_k, w_v):
    weights = (w_q, w_o, w_k, w_v)
    steps = n_rep.bit_length() - 1 + 2
    bf16, f32 = jnp.bfloat16, jnp.float32
    dma = pltpu.SemaphoreType.DMA
    return pl.pallas_call(
        functools.partial(gather_kernel, n_rep),
        out_shape=(jax.ShapeDtypeStruct(count.shape, f32),)
        + tuple(jax.ShapeDtypeStruct((w.shape[0], w.shape[1] * 4), bf16) for w in weights),
        in_specs=[VM] + [ANY] * 4,
        out_specs=(VM,) + (ANY,) * 4,
        scratch_shapes=[pltpu.VMEM(w.shape, bf16) for w in weights]
        + [
            pltpu.VMEM((steps + 1,) + count.shape, f32),
            pltpu.VMEM((steps,) + count.shape, f32),
            dma((steps,)),
            dma((steps,)),
            dma((4,)),
            dma((2, 4, 4)),
            dma((4, 4)),
            dma((4, 4)),
            dma((4, 4)),
            dma((2, 4, 4)),
            dma((2, 4, 4)),
        ],
        compiler_params=pltpu.CompilerParams(
            collective_id=0, has_side_effects=True, vmem_limit_bytes=16 << 20
        ),
        name="gather_weights",
    )(count, *weights)


RELAY_ROWS = 32


def ffn_exchange(own_ref, blocks, part, inbox, outbox, sems, compute, prepare):
    ag_send, ag_recv, rs_send, rs_recv = sems
    section, shard, replica = place()
    far, odd = shard // 2, shard % 2
    middle = (shard == 1) | (shard == 2)
    spots = (shard + 1 - 2 * odd, 2 - far, 3 - 3 * far)
    back = (1 - 2 * odd, 1 - 2 * far, 1 - 2 * far)
    slots = (spots[0] + (4 - spots[0]) * odd, 2 + far * (2 - 3 * odd), spots[2])
    onward = (3 - 2 * shard, 2 * shard - 3, 2 * shard - 3)
    chunks = own_ref.shape[0] // RELAY_ROWS

    def send_own(step):
        return pltpu.make_async_remote_copy(
            src_ref=own_ref,
            dst_ref=blocks.at[shard],
            send_sem=ag_send.at[(step + 1) // 2],
            recv_sem=ag_recv.at[shard],
            device_id=(section, shard + step, replica),
            device_id_type=MESH,
        )

    def pass_on(spot):
        return pltpu.make_async_remote_copy(
            src_ref=blocks.at[spots[spot]],
            dst_ref=blocks.at[spots[spot]],
            send_sem=ag_send.at[2 + spot],
            recv_sem=ag_recv.at[spots[spot]],
            device_id=(section, shard + onward[spot], replica),
            device_id_type=MESH,
        )

    def send_back(spot, chunk):
        rows = pl.ds(chunk * RELAY_ROWS, RELAY_ROWS)
        return pltpu.make_async_remote_copy(
            src_ref=outbox.at[spot, rows, :],
            dst_ref=inbox.at[slots[spot], rows, :],
            send_sem=rs_send.at[spot, chunk],
            recv_sem=rs_recv.at[slots[spot], chunk],
            device_id=(section, shard + back[spot], replica),
            device_id_type=MESH,
        )

    def arrival(slot, chunk):
        rows = pl.ds(chunk * RELAY_ROWS, RELAY_ROWS)
        return pltpu.make_async_remote_copy(
            src_ref=outbox.at[0, rows, :],
            dst_ref=inbox.at[slot, rows, :],
            send_sem=rs_send.at[0, chunk],
            recv_sem=rs_recv.at[slot, chunk],
            device_id=(section, shard + back[0], replica),
            device_id_type=MESH,
        )

    def arrived(spot):
        pass_on(spot).wait_recv()

        @pl.when(middle)
        def _():
            pass_on(spot).start()

    def give(spot, joined):
        for chunk in range(chunks):
            rows = pl.ds(chunk * RELAY_ROWS, RELAY_ROWS)
            total = part[spots[spot], rows, :]
            if joined:
                arrival(spots[spot], chunk).wait_recv()
                total = total + inbox[spots[spot], rows, :].astype(jnp.float32)
            outbox[spot, rows, :] = total.astype(jnp.bfloat16)
            send_back(spot, chunk).start()

    @pl.when(shard < 3)
    def _():
        send_own(1).start()

    @pl.when(shard > 0)
    def _():
        send_own(-1).start()

    prepare()
    blocks[shard] = own_ref[...]
    compute(shard, True)
    arrived(0)

    @pl.when(middle)
    def _():
        arrived(1)

    compute(spots[0], False)

    @pl.when(jnp.logical_not(middle))
    def _():
        give(0, False)
        arrived(1)

    compute(spots[1], False)

    @pl.when(jnp.logical_not(middle))
    def _():
        give(1, False)

    arrived(2)
    compute(spots[2], False)

    @pl.when(jnp.logical_not(middle))
    def _():
        give(2, False)

    @pl.when(middle)
    def _():
        for spot in (1, 2, 0):
            give(spot, True)

    def finish(chunk):
        rows = pl.ds(chunk * RELAY_ROWS, RELAY_ROWS)

        @pl.when(shard > 0)
        def _():
            arrival(shard, chunk).wait_recv()
            part[shard, rows, :] += inbox[shard, rows, :].astype(jnp.float32)

        @pl.when(shard < 3)
        def _():
            arrival(4, chunk).wait_recv()
            part[shard, rows, :] += inbox[4, rows, :].astype(jnp.float32)

        return part[shard, rows, :]

    def settle():
        @pl.when(shard < 3)
        def _():
            send_own(1).wait_send()

        @pl.when(shard > 0)
        def _():
            send_own(-1).wait_send()

        @pl.when(middle)
        def _():
            for spot in range(3):
                pass_on(spot).wait_send()

        for spot in range(3):
            for chunk in range(chunks):
                send_back(spot, chunk).wait_send()

    return finish, settle


def greet_line(partner=None):
    section, shard, replica = place()
    barrier = pltpu.get_barrier_semaphore()

    def signal(peer):
        pl.semaphore_signal(barrier, inc=1, device_id=peer, device_id_type=MESH)

    @pl.when(shard > 0)
    def _():
        signal((section, shard - 1, replica))

    @pl.when(shard < 3)
    def _():
        signal((section, shard + 1, replica))

    if partner is not None:
        signal(partner)
    pl.semaphore_wait(barrier, 1 + shard * (3 - shard) // 2 + int(partner is not None))


def column_copies(pairs, parts, sem, axis):
    copies = []
    for number in range(parts):
        here = []
        for which, (source, target) in enumerate(pairs):
            size = source.shape[axis] // parts
            span = pl.ds(number * size, size)
            cut = (span, slice(None)) if axis == 0 else (slice(None), span)
            here.append(
                pltpu.make_async_copy(source.at[cut], target.at[cut], sem.at[which, number])
            )
        copies.append(here)
    return copies


def ffn_forward_kernel(
    relay,
    normed_ref,
    hidden_ref,
    wg_hbm,
    wu_hbm,
    wd_hbm,
    result_ref,
    relayed_ref,
    spread_hbm,
    gate_hbm,
    up_hbm,
    active_hbm,
    wg,
    wu,
    wd,
    blocks,
    gates,
    ups,
    actives,
    part,
    inbox,
    outbox,
    handed,
    load_sem,
    down_sem,
    ag_send,
    ag_recv,
    rs_send,
    rs_recv,
    store_sem,
    relay_send,
    relay_recv,
):
    f32, bf16 = jnp.float32, jnp.bfloat16
    section, shard, replica = place()
    partner = (1 - section, shard, replica)
    parts = 4
    span = wg.shape[1] // parts
    width = wd.shape[1] // parts
    heads = column_copies(((wg_hbm, wg), (wu_hbm, wu)), parts, load_sem, 1)
    tails = column_copies(((wd_hbm, wd),), parts, down_sem, 1)
    for group in heads + tails:
        for copy in group:
            copy.start()
    greet_line(partner if relay else None)

    def stores(block):
        return [
            pltpu.make_async_copy(source.at[block], target.at[block], store_sem.at[which, block])
            for which, (source, target) in enumerate(
                ((blocks, spread_hbm), (gates, gate_hbm), (ups, up_hbm), (actives, active_hbm))
            )
        ]

    def hidden_part(block, number):
        columns = pl.ds(pl.multiple_of(number * span, 128), span)
        rows = blocks[block]
        gate = jnp.dot(rows, wg[:, columns], preferred_element_type=f32)
        up = jnp.dot(rows, wu[:, columns], preferred_element_type=f32)
        gates[block, :, columns] = gate.astype(bf16)
        ups[block, :, columns] = up.astype(bf16)
        actives[block, :, columns] = (gate * jax.nn.sigmoid(gate) * up).astype(bf16)

    def down_part(block, number):
        columns = pl.ds(pl.multiple_of(number * width, 128), width)
        part[block, :, columns] = jnp.dot(
            actives[block], wd[:, columns], preferred_element_type=f32
        )

    def compute(block, first):
        if first:
            for number in range(parts):
                for copy in heads[number]:
                    copy.wait()
                hidden_part(block, number)
            for number in range(parts):
                for copy in tails[number]:
                    copy.wait()
                down_part(block, number)
        else:
            lax.fori_loop(0, parts, lambda number, _: (hidden_part(block, number), _)[1], 0)
            lax.fori_loop(0, parts, lambda number, _: (down_part(block, number), _)[1], 0)
        for copy in stores(block):
            copy.start()

    finish, settle = ffn_exchange(
        normed_ref,
        blocks,
        part,
        inbox,
        outbox,
        (ag_send, ag_recv, rs_send, rs_recv),
        compute,
        lambda: None,
    )
    relays = []
    for chunk in range(normed_ref.shape[0] // RELAY_ROWS):
        rows = pl.ds(chunk * RELAY_ROWS, RELAY_ROWS)
        total = hidden_ref[rows, :] + finish(chunk)
        result_ref[rows, :] = total
        if relay:
            handed[rows, :] = total.astype(bf16)
            copy = pltpu.make_async_remote_copy(
                src_ref=handed.at[rows, :],
                dst_ref=relayed_ref.at[rows, :],
                send_sem=relay_send.at[chunk],
                recv_sem=relay_recv.at[chunk],
                device_id=partner,
                device_id_type=MESH,
            )
            copy.start()
            relays.append(copy)
    settle()
    for block in range(4):
        for copy in stores(block):
            copy.wait()
    for copy in relays:
        copy.wait()
    if not relay:
        relayed_ref[...] = jnp.zeros_like(relayed_ref)


def ffn_scratch(rows, width, span):
    f32, bf16 = jnp.float32, jnp.bfloat16
    dma = pltpu.SemaphoreType.DMA
    chunks = rows // RELAY_ROWS
    weights = [
        pltpu.VMEM((width, span), bf16),
        pltpu.VMEM((width, span), bf16),
        pltpu.VMEM((span, width), bf16),
    ]
    row_blocks = [
        pltpu.VMEM((4, rows, width), bf16),
        pltpu.VMEM((4, rows, span), bf16),
        pltpu.VMEM((4, rows, span), bf16),
        pltpu.VMEM((4, rows, span), bf16),
    ]
    sums = [
        pltpu.VMEM((4, rows, width), f32),
        pltpu.VMEM((5, rows, width), bf16),
        pltpu.VMEM((3, rows, width), bf16),
    ]
    sems = [dma((5,)), dma((4,)), dma((3, chunks)), dma((5, chunks))]
    return weights, row_blocks, sums, sems


def ffn_cost(rows, width, span):
    return pl.CostEstimate(
        flops=3 * 2 * 4 * rows * width * span,
        bytes_accessed=3 * 2 * width * span + 16 * 2 * rows * width,
        transcendentals=4 * rows * span,
    )


def ffn_forward(relay, normed, hidden, w_g, w_u, w_d):
    f32, bf16 = jnp.float32, jnp.bfloat16
    rows, width = normed.shape
    span = w_g.shape[1]
    dma = pltpu.SemaphoreType.DMA
    chunks = rows // RELAY_ROWS
    weights, row_blocks, sums, sems = ffn_scratch(rows, width, span)
    return pl.pallas_call(
        functools.partial(ffn_forward_kernel, relay),
        out_shape=(
            jax.ShapeDtypeStruct((rows, width), f32),
            jax.ShapeDtypeStruct((rows, width), bf16),
            jax.ShapeDtypeStruct((4, rows, width), bf16),
        )
        + (jax.ShapeDtypeStruct((4, rows, span), bf16),) * 3,
        in_specs=[VM, VM, ANY, ANY, ANY],
        out_specs=(VM, VM, ANY, ANY, ANY, ANY),
        scratch_shapes=weights
        + row_blocks
        + sums
        + [pltpu.VMEM((rows, width), bf16), dma((2, 4)), dma((1, 4))]
        + sems
        + [dma((4, 4)), dma((chunks,)), dma((chunks,))],
        compiler_params=pltpu.CompilerParams(
            collective_id=2 + int(relay), has_side_effects=True, vmem_limit_bytes=56 << 20
        ),
        cost_estimate=ffn_cost(rows, width, span),
        name="ffn_forward",
    )(normed, hidden, w_g, w_u, w_d)


def ffn_backward_kernel(
    grad_ref,
    wg_hbm,
    wu_hbm,
    wd_hbm,
    gate_zero,
    up_zero,
    gate_one,
    up_one,
    normed_ref,
    rows_hbm,
    ggate_hbm,
    gup_hbm,
    wg,
    wu,
    wd,
    blocks,
    gates,
    ups,
    part,
    inbox,
    outbox,
    load_sem,
    down_sem,
    ag_send,
    ag_recv,
    rs_send,
    rs_recv,
    store_sem,
    kept_sem,
):
    f32, bf16 = jnp.float32, jnp.bfloat16
    section, shard, replica = place()
    parts = 4
    span = wg.shape[1] // parts
    width = wg.shape[0] // parts
    heads = column_copies(((wd_hbm, wd),), parts, down_sem, 0)
    tails = column_copies(((wg_hbm, wg), (wu_hbm, wu)), parts, load_sem, 0)

    def kept(gate, up):
        return [
            pltpu.make_async_copy(gate, gates, kept_sem.at[0]),
            pltpu.make_async_copy(up, ups, kept_sem.at[1]),
        ]

    @pl.when(section == 0)
    def _():
        for copy in kept(gate_zero, up_zero):
            copy.start()

    @pl.when(section == 1)
    def _():
        for copy in kept(gate_one, up_one):
            copy.start()

    for group in heads + tails:
        for copy in group:
            copy.start()
    greet_line()

    def stores(block):
        return [
            pltpu.make_async_copy(source.at[block], target.at[block], store_sem.at[which, block])
            for which, (source, target) in enumerate(
                ((blocks, rows_hbm), (gates, ggate_hbm), (ups, gup_hbm))
            )
        ]

    def hidden_part(block, number):
        start = pl.multiple_of(number * span, 128)
        columns = pl.ds(start, span)
        grad = across(blocks[block], wd[pl.ds(start, span), :])
        gate = gates[block, :, columns].astype(f32)
        up = ups[block, :, columns].astype(f32)
        sigma = jax.nn.sigmoid(gate)
        gates[block, :, columns] = (grad * up * sigma * (1.0 + gate * (1.0 - sigma))).astype(bf16)
        ups[block, :, columns] = (grad * gate * sigma).astype(bf16)

    def input_part(block, number):
        start = pl.multiple_of(number * width, 128)
        columns = pl.ds(start, width)
        part[block, :, columns] = across(gates[block], wg[pl.ds(start, width), :]) + across(
            ups[block], wu[pl.ds(start, width), :]
        )

    def compute(block, first):
        if first:
            for number in range(parts):
                for copy in heads[number]:
                    copy.wait()
                hidden_part(block, number)
            for number in range(parts):
                for copy in tails[number]:
                    copy.wait()
                input_part(block, number)
        else:
            lax.fori_loop(0, parts, lambda number, _: (hidden_part(block, number), _)[1], 0)
            lax.fori_loop(0, parts, lambda number, _: (input_part(block, number), _)[1], 0)
        for copy in stores(block):
            copy.start()

    def prepare():
        for copy in kept(gate_zero, up_zero):
            copy.wait()

    finish, settle = ffn_exchange(
        grad_ref,
        blocks,
        part,
        inbox,
        outbox,
        (ag_send, ag_recv, rs_send, rs_recv),
        compute,
        prepare,
    )
    for chunk in range(grad_ref.shape[0] // RELAY_ROWS):
        rows = pl.ds(chunk * RELAY_ROWS, RELAY_ROWS)
        normed_ref[rows, :] = finish(chunk)
    settle()
    for block in range(4):
        for copy in stores(block):
            copy.wait()


def ffn_backward(grad, w_g, w_u, w_d, kept_zero, kept_one):
    f32, bf16 = jnp.float32, jnp.bfloat16
    rows, width = grad.shape
    span = w_g.shape[1]
    dma = pltpu.SemaphoreType.DMA
    weights, row_blocks, sums, sems = ffn_scratch(rows, width, span)
    row_blocks = row_blocks[:3]
    return pl.pallas_call(
        ffn_backward_kernel,
        out_shape=(
            jax.ShapeDtypeStruct((rows, width), f32),
            jax.ShapeDtypeStruct((4, rows, width), bf16),
        )
        + (jax.ShapeDtypeStruct((4, rows, span), bf16),) * 2,
        in_specs=[VM] + [ANY] * 7,
        out_specs=(VM, ANY, ANY, ANY),
        scratch_shapes=weights
        + row_blocks
        + sums
        + [dma((2, 4)), dma((1, 4))]
        + sems
        + [dma((3, 4)), dma((2,))],
        compiler_params=pltpu.CompilerParams(
            collective_id=4, has_side_effects=True, vmem_limit_bytes=56 << 20
        ),
        cost_estimate=ffn_cost(rows, width, span),
        name="ffn_backward",
    )(grad, w_g, w_u, w_d, *kept_zero, *kept_one)


def sum_kernel(n_rep, part_ref, group_out, whole_out, totals, heard, send_sem, recv_sem):
    section, shard, replica = place()
    peers = reduce_peers(n_rep) + [(1 - section, shard, replica)]
    greet(peers)
    totals[0] = part_ref[...]
    butterfly(peers, totals, heard, send_sem, recv_sem)
    group_out[...] = totals[len(peers) - 1]
    whole_out[...] = totals[len(peers)]


def small_sums(n_rep, part):
    steps = n_rep.bit_length() - 1 + 3
    shape = jax.ShapeDtypeStruct(part.shape, jnp.float32)
    return pl.pallas_call(
        functools.partial(sum_kernel, n_rep),
        out_shape=(shape, shape),
        in_specs=[VM],
        out_specs=(VM, VM),
        scratch_shapes=[
            pltpu.VMEM((steps + 1,) + part.shape, jnp.float32),
            pltpu.VMEM((steps,) + part.shape, jnp.float32),
            pltpu.SemaphoreType.DMA((steps,)),
            pltpu.SemaphoreType.DMA((steps,)),
        ],
        compiler_params=pltpu.CompilerParams(
            collective_id=1, has_side_effects=True, vmem_limit_bytes=8 << 20
        ),
        name="small_sums",
    )(part)


def flip(block, bit):
    size = lax.axis_size("replica")
    return lax.ppermute(block, "replica", [(i, i ^ bit) for i in range(size)])


def alternate(array, which, length, axis):
    count = array.shape[axis] // (2 * length)
    pieces = [
        lax.dynamic_slice_in_dim(array, (2 * k + which) * length, length, axis)
        for k in range(count)
    ]
    return pieces[0] if count == 1 else jnp.concatenate(pieces, axis)


def half_blocks(array, which, axis=1):
    length = array.shape[axis] // lax.axis_size("replica")
    return alternate(array, which, 2 * length, axis)


def owned(lefts, rights, split):
    size = lax.axis_size("replica")
    me = lax.axis_index("replica")
    left, right = jnp.concatenate(lefts), jnp.concatenate(rights)
    divided = right if split else left
    length = divided.shape[1] * 2 // size

    def product(which):
        chosen = alternate(divided, which, length, 1)
        return down_rows(left, chosen) if split else down_rows(chosen, right)

    arrived = flip(product(1 - (me & 1)).astype(jnp.bfloat16), 1)
    total = product(me & 1) + arrived.astype(jnp.float32)
    bit = 4
    while bit < size:
        here = (me // bit) & 1
        arrived = flip(alternate(total, 1 - here, length, split).astype(jnp.bfloat16), bit)
        total = alternate(total, here, length, split) + arrived.astype(jnp.float32)
        bit *= 2
    return total


def met(array):
    return [array, flip(array, 2)]


def met_half(array):
    here = (lax.axis_index("replica") // 2) & 1
    return [half_blocks(array, here), flip(half_blocks(array, 1 - here), 2)]


def over_shard(grad):
    return lax.psum_scatter(
        grad.astype(jnp.bfloat16), "shard", scatter_dimension=1, tiled=True
    ).astype(jnp.float32)


def per_device(
    tokens,
    targets,
    deal,
    lengths,
    attn_gain,
    w_query,
    w_key,
    w_value,
    w_out,
    ffn_gain,
    w_gate,
    w_up,
    w_down,
):
    f32 = jnp.float32
    bf16 = jnp.bfloat16
    n_rep = lax.axis_size("replica")
    section_id = lax.axis_index("section")
    later = section_id == 1
    micro_count = lengths.shape[0]
    row_count = tokens.shape[0] // micro_count
    model_width = tokens.shape[1]
    group_size = H // KV
    score_scale = HD ** (-0.5)
    arrival = deal[0]
    slot_inputs = tokens[arrival].reshape(micro_count, row_count, model_width)
    teacher = targets[arrival].astype(f32)
    gain_attn = attn_gain[0].astype(f32)
    gain_ffn = ffn_gain[0].astype(f32)
    local_count = jnp.broadcast_to(jnp.sum(lengths).astype(f32), (8, 128))
    counted, w_q, w_o, w_k, w_v = gather_weights(
        n_rep, local_count, w_query[0], w_out[0], w_key[0], w_value[0]
    )
    total_count = counted[0, 0]
    w_g, w_u, w_d = (w_gate[0], w_up[0], w_down[0])
    received = jnp.zeros((row_count, model_width), bf16)
    outputs_seen = []
    kept_seen = []
    ffn_seen = []

    def pick(one, zero):
        return jax.tree.map(lambda a, b: jnp.where(later, a, b), one, zero)

    for moment in range(micro_count + 1):
        own_batch = jnp.clip(moment - section_id, 0, micro_count - 1)
        fresh = lax.dynamic_index_in_dim(slot_inputs, own_batch, 0, keepdims=False)
        seq_lengths = lax.dynamic_index_in_dim(lengths, own_batch, 0, keepdims=False)
        rows_in = jnp.where(later, received, fresh).astype(f32)
        forward_allowed, forward_cosine, forward_sine = attend_mask(seq_lengths, row_count)
        forward_inverse_one = lax.rsqrt(jnp.mean(rows_in * rows_in, axis=1, keepdims=True) + EPS)
        forward_normed_one = (rows_in * forward_inverse_one * gain_attn).astype(bf16)
        query = jnp.dot(forward_normed_one, w_q, preferred_element_type=f32).reshape(
            row_count, H, HD
        )
        keys = jnp.dot(forward_normed_one, w_k, preferred_element_type=f32).reshape(
            row_count, KV, HD
        )
        forward_values = (
            jnp.dot(forward_normed_one, w_v, preferred_element_type=f32)
            .astype(bf16)
            .reshape(row_count, KV, HD)
        )
        forward_q_rot = (
            rotate(query, forward_cosine, forward_sine)
            .astype(bf16)
            .reshape(row_count, KV, group_size, HD)
        )
        forward_k_rot = rotate(keys, forward_cosine, forward_sine).astype(bf16)
        forward_scores = (
            jnp.einsum("rkgd,skd->kgrs", forward_q_rot, forward_k_rot, preferred_element_type=f32)
            * score_scale
        )
        forward_scores = jnp.where(forward_allowed, forward_scores, NEG)
        highest = jnp.max(forward_scores, axis=-1, keepdims=True)
        raised = jnp.exp(forward_scores - highest)
        totals = jnp.sum(raised, axis=-1, keepdims=True)
        forward_probs = (raised / totals).astype(bf16)
        forward_log_total = highest + jnp.log(totals)
        forward_mixed = jnp.einsum(
            "kgrs,skd->rkgd", forward_probs, forward_values, preferred_element_type=f32
        )
        forward_mixed = forward_mixed.reshape(row_count, H * HD).astype(bf16)
        forward_hidden = rows_in + jnp.dot(forward_mixed, w_o, preferred_element_type=f32)
        forward_inverse_two = lax.rsqrt(
            jnp.mean(forward_hidden * forward_hidden, axis=1, keepdims=True) + EPS
        )
        forward_normed_two = (forward_hidden * forward_inverse_two * gain_ffn).astype(bf16)
        result, received, *ffn_kept = ffn_forward(
            moment < micro_count, forward_normed_two, forward_hidden, w_g, w_u, w_d
        )
        forward_kept = (
            rows_in.astype(bf16),
            forward_inverse_one,
            forward_normed_one,
            forward_q_rot,
            forward_k_rot,
            forward_values,
            forward_log_total,
            forward_mixed,
            forward_hidden,
            forward_inverse_two,
        )
        outputs_seen.append(result)
        kept_seen.append(forward_kept)
        ffn_seen.append(ffn_kept)
    kept_sets = (pick(kept_seen[2], kept_seen[0]), kept_seen[1])
    ffn_sets = (pick(ffn_seen[2], ffn_seen[0]), ffn_seen[1])
    normed_met, mixed_met, spread_met, active_met = [], [], [], []
    for kept, ffn_kept in zip(kept_sets[::-1], ffn_sets[::-1]):
        spread_met += met_half(ffn_kept[0].reshape(-1, model_width))
        active_met += met(ffn_kept[3].reshape(-1, ffn_kept[3].shape[-1]))
        here = (lax.axis_index("replica") // 2) & 1
        normed, mixed = kept[2], kept[7]
        away = flip(
            jnp.concatenate([half_blocks(normed, 1 - here), half_blocks(mixed, 1 - here)], axis=1), 2
        )
        normed_met += [half_blocks(normed, here), away[:, : normed.shape[1] // 2]]
        mixed_met += [half_blocks(mixed, here), away[:, normed.shape[1] // 2 :]]
    mine = jnp.concatenate(
        [pick(outputs_seen[batch + 1], outputs_seen[batch]) for batch in range(micro_count)]
    )
    segments_all = jax.vmap(lambda seq_lengths: layout(seq_lengths, row_count)[0])(lengths)
    valid_rows = (segments_all < lengths.shape[1]).reshape(-1).astype(f32)[:, None]
    errors = mine - teacher
    switch = later.astype(f32)
    local_square = jnp.sum(valid_rows * errors * errors) * switch
    all_tokens = tokens.shape[0] * lax.axis_size("shard") * lax.axis_size("replica")
    grad_final = (all_tokens / total_count * errors * valid_rows).reshape(
        micro_count, row_count, model_width
    )
    coming = jnp.zeros((row_count, model_width), bf16)
    sent_seen = []
    stored_seen = []
    gain_attn_total = jnp.zeros((model_width,), f32)
    gain_ffn_total = jnp.zeros((model_width,), f32)
    for moment in range(micro_count + 1):
        raw_batch = moment - 1 + section_id
        own_batch = jnp.clip(raw_batch, 0, micro_count - 1)
        if moment == 1:
            kept = kept_sets[0]
            ffn_zero, ffn_one = ffn_seen[0], ffn_seen[2]
        else:
            kept = kept_seen[1]
            ffn_zero, ffn_one = ffn_seen[1], ffn_seen[1]
        seq_lengths = lax.dynamic_index_in_dim(lengths, own_batch, 0, keepdims=False)
        final_rows = lax.dynamic_index_in_dim(grad_final, own_batch, 0, keepdims=False)
        incoming = jnp.where(later, final_rows, coming.astype(f32))
        (
            input_rows,
            inverse_one,
            normed_one,
            q_rot,
            k_rot,
            values,
            log_total,
            mixed,
            hidden,
            inverse_two,
        ) = kept
        allowed, cosine, sine = attend_mask(seq_lengths, row_count)
        grad_normed, backward_grad_rows, backward_grad_gate, backward_grad_up = ffn_backward(
            incoming.astype(bf16), w_g, w_u, w_d, ffn_zero[1:3], ffn_one[1:3]
        )
        scaled_two = hidden * inverse_two
        gain_ffn_part = jnp.sum(grad_normed * scaled_two, axis=0)
        pushed_two = grad_normed * gain_ffn
        grad_hidden = incoming + inverse_two * (
            pushed_two - scaled_two * jnp.mean(pushed_two * scaled_two, axis=1, keepdims=True)
        )
        backward_grad_attn = grad_hidden.astype(bf16)
        grad_mixed = (
            across(backward_grad_attn, w_o).astype(bf16).reshape(row_count, KV, group_size, HD)
        )
        scores = (
            jnp.einsum("rkgd,skd->kgrs", q_rot, k_rot, preferred_element_type=f32) * score_scale
        )
        probs = jnp.where(allowed, jnp.exp(scores - log_total), 0.0)
        grad_probs = jnp.einsum("rkgd,skd->kgrs", grad_mixed, values, preferred_element_type=f32)
        grad_scores = (
            probs * (grad_probs - jnp.sum(grad_probs * probs, axis=-1, keepdims=True))
        ).astype(bf16)
        grad_qrot = (
            jnp.einsum("kgrs,skd->rkgd", grad_scores, k_rot, preferred_element_type=f32)
            * score_scale
        )
        grad_krot = (
            jnp.einsum("kgrs,rkgd->skd", grad_scores, q_rot, preferred_element_type=f32)
            * score_scale
        )
        backward_grad_values = jnp.einsum(
            "kgrs,rkgd->skd", probs.astype(bf16), grad_mixed, preferred_element_type=f32
        )
        backward_grad_values = backward_grad_values.astype(bf16).reshape(row_count, KV * HD)
        backward_grad_query = (
            rotate_back(grad_qrot.reshape(row_count, H, HD), cosine, sine)
            .astype(bf16)
            .reshape(row_count, H * HD)
        )
        backward_grad_keys = (
            rotate_back(grad_krot, cosine, sine).astype(bf16).reshape(row_count, KV * HD)
        )
        grad_normed_one = (
            across(backward_grad_query, w_q)
            + across(backward_grad_keys, w_k)
            + across(backward_grad_values, w_v)
        )
        scaled_one = input_rows.astype(f32) * inverse_one
        gain_attn_part = jnp.sum(grad_normed_one * scaled_one, axis=0)
        pushed_one = grad_normed_one * gain_attn
        grad_input = grad_hidden + inverse_one * (
            pushed_one - scaled_one * jnp.mean(pushed_one * scaled_one, axis=1, keepdims=True)
        )
        grads = tuple(
            stack.reshape(-1, stack.shape[-1])
            for stack in (backward_grad_gate, backward_grad_up, backward_grad_rows)
        )
        projected = jnp.concatenate(
            [backward_grad_query, backward_grad_keys, backward_grad_values], axis=1
        )
        active_moment = (raw_batch >= 0) & (raw_batch < micro_count)
        gain_attn_total = gain_attn_total + jnp.where(active_moment, gain_attn_part, 0.0)
        gain_ffn_total = gain_ffn_total + jnp.where(active_moment, gain_ffn_part, 0.0)
        sent = grad_input.astype(bf16)
        if moment < micro_count:
            coming = from_behind(sent, "section", -1)
        sent_seen.append(sent)
        stored_seen.append((projected, backward_grad_attn) + grads)
    grads_in = jnp.concatenate(
        [pick(sent_seen[batch], sent_seen[batch + 1]) for batch in range(micro_count)]
    )
    stored_sets = (stored_seen[1], pick(stored_seen[0], stored_seen[2]))
    projected_met, attn_met, gate_met, up_met, rows_met = [], [], [], [], []
    for projected, grad_attn, grad_gate, grad_up, grad_rows in stored_sets[::-1]:
        rows_met += met_half(grad_rows)
        gate_met += met(grad_gate)
        up_met += met(grad_up)
        attn_met += met(grad_attn)
        projected_met += met(projected)
    small = jnp.stack([gain_attn_total, gain_ffn_total])
    small = jnp.concatenate([small, jnp.broadcast_to(local_square, (6, model_width))])
    group_sums, whole_sums = small_sums(n_rep, small)
    down_grad = owned(active_met, rows_met, 1)
    gate_grad = owned(spread_met, gate_met, 0)
    up_grad = owned(spread_met, up_met, 0)
    out_grad = over_shard(owned(mixed_met, attn_met, 0))
    projected_grad = owned(normed_met, projected_met, 0)
    query_width, key_width = H * HD, KV * HD
    query_grad = over_shard(projected_grad[:, :query_width])
    key_grad = over_shard(projected_grad[:, query_width : query_width + key_width])
    value_grad = over_shard(projected_grad[:, query_width + key_width :])
    loss_value = whole_sums[2, 0] / (total_count * model_width)
    share = model_width // (lax.axis_size("shard") * n_rep)
    start = (lax.axis_index("shard") * n_rep + lax.axis_index("replica")) * share
    attn_gain_part = lax.dynamic_slice_in_dim(group_sums[0], start, share, 0)
    ffn_gain_part = lax.dynamic_slice_in_dim(group_sums[1], start, share, 0)
    outputs_local = (
        jnp.zeros((tokens.shape[0], model_width), bf16).at[arrival].set(mine.astype(bf16))[None]
    )
    input_local = jnp.zeros((tokens.shape[0], model_width), bf16).at[arrival].set(grads_in)[None]
    return (
        loss_value,
        outputs_local,
        input_local,
        attn_gain_part[None],
        query_grad[None],
        key_grad[None],
        value_grad[None],
        out_grad[None],
        ffn_gain_part[None],
        gate_grad[None],
        up_grad[None],
        down_grad[None],
    )


def solution(mesh):
    in_specs = (
        P(("shard", "replica"), None),
        P(("shard", "replica"), None),
        P(("shard", "replica"), None),
        P(("shard", "replica"), None),
        P("section", None),
        P("section", None, "shard"),
        P("section", None, "shard"),
        P("section", None, "shard"),
        P("section", None, "shard"),
        P("section", None),
        P("section", None, "shard"),
        P("section", None, "shard"),
        P("section", "shard", None),
    )
    out_specs = (
        P(),
        P("section", ("shard", "replica"), None),
        P("section", ("shard", "replica"), None),
        P("section", ("shard", "replica")),
        P("section", "replica", "shard"),
        P("section", "replica", "shard"),
        P("section", "replica", "shard"),
        P("section", "replica", "shard"),
        P("section", ("shard", "replica")),
        P("section", "replica", "shard"),
        P("section", "replica", "shard"),
        P("section", "shard", "replica"),
    )
    return jax.shard_map(
        per_device, mesh=mesh, in_specs=in_specs, out_specs=out_specs, check_vma=False
    )
```
